32 devices in a mesh: row: 8 (over y, x, core), col: 4 (over z).
Axes of the slice: x: 2, y: 2, z: 4, core: 2. Of those that a mesh axis runs over, the one named last changes fastest.
Arguments:
- tangents: float32 [192, 128, 6144], P('row', None, 'col'), may hold values from -6 to 6
- base_flow: float32 [192, 128, 192], P('row', None, 'col'), may hold values from -0.0625 to 0.0625
- mode_mask: int32 [192, 192], P('row', 'col'), may hold values 0 or 1
- decay_rates: float32 [128], replicated, may hold values from 1 to 100
- to_eigen: float32 [128, 128], replicated, may hold values from -0.5 to 0.5
- from_eigen: float32 [128, 128], replicated, may hold values from -0.5 to 0.5
Outputs:
- vectors: float32 [192, 128, 6144], P('row', None, 'col')
- growth: float32 [32], replicated
The draws below stay inside these ranges and needn't reach their ends.
Inputs may be any that keep to these rules, and one draw needn't show every extreme that they name: `mode_mask`: 1 keeps a mode pair of the linearized product, 0 removes it.
All inputs are finite; a program needn't handle non-finite values. No bound on the sum of `mode_mask` on one device may be relied on, other than what follows from the above.
Results may differ from the reference program's by a relative error of at most 0.00005.
Values sent between devices are 32-bit elements; how exact they have to be, the bound alone decides.
A program may use at most 256 MiB of HBM per device.

```python
import math
import jax
import jax.numpy as jnp
from jax import lax

NX = 192
NY = 128
NZ = 192
NV = 32


def plant(values, rng, least, top_value):
    longest = values.shape.index(max(values.shape))
    spots = []
    for shift in (0, 1):
        where = [jax.random.randint(jax.random.fold_in(rng, axis), (), 0, length) for axis, length in enumerate(values.shape)]
        where[longest] = (where[longest] + shift) % values.shape[longest]
        spots.append(tuple(where))
    return values.at[spots[0]].set(least).at[spots[1]].set(top_value)


def block_scale(rng, shape, pieces, least, high):
    factor_of, own = 1.0, jax.random.fold_in(rng, 6)
    for axis_at, parts in pieces:
        heights = jnp.exp(jax.random.uniform(jax.random.fold_in(own, axis_at), (parts,), jnp.float32, least / len(pieces), high / len(pieces)))
        factor_of = factor_of * jnp.repeat(heights, shape[axis_at] // parts).reshape([-1 if axis == axis_at else 1 for axis in range(len(shape))])
    return factor_of


def centred(rng, dims, deviation, most, cuts=(), kind=jnp.bfloat16):
    drawn = deviation * jax.random.normal(rng, dims, jnp.float32)
    if cuts:
        drawn = drawn * block_scale(rng, dims, cuts, -0.22, 0.18)
    return jnp.clip(drawn, -most, most).astype(kind)


def setup_inputs(seed: int = 0) -> dict:
    key_list = jax.random.split(jax.random.key(seed), 7)
    tangents = centred(key_list[0], (NX, NY, NZ * NV), 1.0, 6.0, ((0, 8), (2, 4)), jnp.float32)
    base_flow = centred(key_list[1], (NX, NY, NZ), (NX * NZ // 4) ** -0.5, 0.0625, ((0, 8), (2, 4)), jnp.float32)
    mode_mask = plant((jax.random.randint(key_list[2], (NX, NZ), 0, 4) < 3).astype(jnp.int32), jax.random.fold_in(key_list[2], 1), 0, 1)
    decay_rates = jnp.clip(jnp.exp(jax.random.uniform(key_list[3], (NY,), jnp.float32, math.log(1.0), math.log(100.0))), 1.0, 100.0)
    to_eigen = centred(key_list[4], (NY, NY), NY ** -0.5, 0.5, (), jnp.float32)
    from_eigen = centred(key_list[5], (NY, NY), NY ** -0.5, 0.5, (), jnp.float32)
    return dict(tangents=tangents, base_flow=base_flow, mode_mask=mode_mask, decay_rates=decay_rates, to_eigen=to_eigen, from_eigen=from_eigen)


PRECISE = lax.Precision.HIGHEST
STEP_COEF = 10.0
VISCOSITY = 0.01
ALPHA_X = 0.5
BETA_Z = 1.0

def local_waves(points_count, first_index, length):
    indices = first_index + jnp.arange(length, dtype=jnp.int32)
    middle = points_count // 2
    return jnp.where(indices <= middle, indices, indices - middle).astype(jnp.float32)

def synthesis(points_count):
    points = jnp.arange(points_count, dtype=jnp.int32)[:, None]
    mode_index = jnp.arange(points_count, dtype=jnp.int32)[None, :]
    middle = points_count // 2
    wave_index = jnp.where(mode_index <= middle, mode_index, mode_index - middle)
    turn_count = (points * wave_index % points_count).astype(jnp.float32)
    angles = turn_count * (2.0 * math.pi / points_count)
    return jnp.where(mode_index <= middle, jnp.cos(angles), jnp.sin(angles))

def analysis(points_count):
    mode_index = jnp.arange(points_count, dtype=jnp.int32)
    middle = points_count // 2
    weights = jnp.where((mode_index == 0) | (mode_index == middle), jnp.float32(1.0 / points_count), jnp.float32(2.0 / points_count))
    return weights[:, None] * synthesis(points_count).T

def derivative_analysis(points_count, wave_scale):
    rows_index = jnp.arange(points_count, dtype=jnp.int32)[:, None]
    cols_index = jnp.arange(points_count, dtype=jnp.int32)[None, :]
    middle = points_count // 2
    rising = (cols_index == rows_index + middle) & (rows_index >= 1) & (rows_index < middle)
    falling = (rows_index == cols_index + middle) & (cols_index >= 1) & (cols_index < middle)
    rows_float = jnp.broadcast_to(rows_index.astype(jnp.float32), (points_count, points_count))
    cols_float = jnp.broadcast_to(cols_index.astype(jnp.float32), (points_count, points_count))
    derivative = jnp.where(rising, rows_float, jnp.float32(0.0)) - jnp.where(falling, cols_float, jnp.float32(0.0))
    return -wave_scale * jnp.dot(derivative, analysis(points_count), precision=PRECISE)

def denominators(decay_rates, x_count, z_count, x_start, z_start, x_length, z_length):
    wave_x = ALPHA_X * local_waves(x_count, x_start, x_length)
    wave_z = BETA_Z * local_waves(z_count, z_start, z_length)
    return STEP_COEF + VISCOSITY * (wave_x[:, None, None] ** 2 + wave_z[None, None, :] ** 2) + decay_rates[None, :, None]

def reference(tangents, base_flow, mode_mask, decay_rates, to_eigen, from_eigen):
    x_count, y_count, z_count = base_flow.shape
    vec_count = tangents.shape[2] // z_count
    fields = jnp.transpose(tangents.reshape(x_count, y_count, z_count, vec_count), (3, 0, 1, 2))
    x_synthesis = synthesis(x_count)
    z_synthesis = synthesis(z_count)
    x_derivative = derivative_analysis(x_count, ALPHA_X)
    z_analysis = analysis(z_count)
    speed_field = jnp.einsum('pm,myn->pyn', x_synthesis, base_flow, precision=PRECISE)
    speed_field = jnp.einsum('pyn,sn->pys', speed_field, z_synthesis, precision=PRECISE)
    divisor = denominators(decay_rates, x_count, z_count, 0, 0, x_count, z_count)
    retained = mode_mask.astype(jnp.float32)[:, None, :]

    def advance(one_field):
        physical = jnp.einsum('pm,myn->pyn', x_synthesis, one_field, precision=PRECISE)
        physical = jnp.einsum('pyn,sn->pys', physical, z_synthesis, precision=PRECISE)
        product = speed_field * physical
        returned = jnp.einsum('mp,pys->mys', x_derivative, product, precision=PRECISE)
        returned = jnp.einsum('mys,ns->myn', returned, z_analysis, precision=PRECISE)
        right_side = STEP_COEF * one_field + retained * returned
        eigen_part = jnp.einsum('ji,min->mjn', to_eigen, right_side, precision=PRECISE) / divisor
        return jnp.einsum('yj,mjn->myn', from_eigen, eigen_part, precision=PRECISE)
    stepped = lax.map(advance, fields)
    cell_count = x_count * y_count * z_count
    gram_matrix = jnp.einsum('vmyn,umyn->vu', stepped, stepped, precision=PRECISE) / cell_count
    lower_factor = jnp.linalg.cholesky(gram_matrix)
    identity = jnp.eye(vec_count, dtype=jnp.float32)
    inverse = jax.scipy.linalg.solve_triangular(lower_factor, identity, lower=True)
    orthonormal = jnp.einsum('uv,vmyn->mynu', inverse, stepped, precision=PRECISE)
    growth = jnp.log(jnp.diagonal(lower_factor))
    return (orthonormal.reshape(x_count, y_count, z_count * vec_count), growth)
```

```python
import functools
import math

import jax
import jax.numpy as jnp
from jax import lax
from jax.experimental import pallas as pl
from jax.experimental.pallas import tpu as pltpu
from jax.sharding import PartitionSpec as P

PRECISE = lax.Precision.HIGHEST
STEP_COEF = 10.0
VISCOSITY = 0.01
ALPHA_X = 0.5
BETA_Z = 1.0


def local_waves(points_count, first_index, length):
    indices = first_index + jnp.arange(length, dtype=jnp.int32)
    middle = points_count // 2
    return jnp.where(indices <= middle, indices, indices - middle).astype(jnp.float32)


def synthesis(points_count):
    points = jnp.arange(points_count, dtype=jnp.int32)[:, None]
    mode_index = jnp.arange(points_count, dtype=jnp.int32)[None, :]
    middle = points_count // 2
    wave_index = jnp.where(mode_index <= middle, mode_index, mode_index - middle)
    turn_count = (points * wave_index % points_count).astype(jnp.float32)
    angles = turn_count * (2.0 * math.pi / points_count)
    return jnp.where(mode_index <= middle, jnp.cos(angles), jnp.sin(angles))


def analysis(points_count):
    mode_index = jnp.arange(points_count, dtype=jnp.int32)
    middle = points_count // 2
    weights = jnp.where(
        (mode_index == 0) | (mode_index == middle),
        jnp.float32(1.0 / points_count),
        jnp.float32(2.0 / points_count),
    )
    return weights[:, None] * synthesis(points_count).T


def derivative_analysis(points_count, wave_scale):
    rows_index = jnp.arange(points_count, dtype=jnp.int32)[:, None]
    cols_index = jnp.arange(points_count, dtype=jnp.int32)[None, :]
    middle = points_count // 2
    rising = (cols_index == rows_index + middle) & (rows_index >= 1) & (rows_index < middle)
    falling = (rows_index == cols_index + middle) & (cols_index >= 1) & (cols_index < middle)
    rows_float = jnp.broadcast_to(rows_index.astype(jnp.float32), (points_count, points_count))
    cols_float = jnp.broadcast_to(cols_index.astype(jnp.float32), (points_count, points_count))
    derivative = jnp.where(rising, rows_float, jnp.float32(0.0)) - jnp.where(
        falling, cols_float, jnp.float32(0.0)
    )
    return -wave_scale * jnp.dot(derivative, analysis(points_count), precision=PRECISE)


def split_parts(value):
    high = value.astype(jnp.bfloat16)
    low = (value - high.astype(jnp.float32)).astype(jnp.bfloat16)
    return high, low


def parts_dot(left, right):
    left_high, left_low = left
    right_high, right_low = right
    dot = lambda a, b: jnp.dot(a, b, preferred_element_type=jnp.float32)
    return dot(left_high, right_high) + (dot(left_high, right_low) + dot(left_low, right_high))


def plane_kernel(vec_count, x_ref, speed_ref, sx_ref, sz_ref, az_ref, gx_ref, o_ref, rows, *halves):
    row_devices, col_devices, x_length, zv_length = x_ref.shape
    x_count = row_devices * x_length
    z_count = sz_ref.shape[0]
    if rows.shape[0] > x_count:
        rows[x_count:, :] = jnp.zeros((rows.shape[0] - x_count, zv_length), jnp.float32)
    for c in range(col_devices):
        for r in range(row_devices):
            rows[r * x_length : (r + 1) * x_length, :] = x_ref[r, c]
        for h, half in enumerate(halves):
            half[c * zv_length : (c + 1) * zv_length, :] = rows[h * 128 : (h + 1) * 128, :].T
    sx = split_parts(sx_ref[...])
    sz = split_parts(sz_ref[...])
    az = split_parts(az_ref[...])
    gx = split_parts(gx_ref[...])

    def step(group, carry):
        for u in range(2):
            where = pl.ds(group * 2 + u, z_count, stride=vec_count)
            field = jnp.concatenate([half[where, :] for half in halves], axis=1)
            field = parts_dot(split_parts(field), sx)
            field = parts_dot(sz, split_parts(field))
            field = field * speed_ref[...]
            field = parts_dot(az, split_parts(field))
            field = parts_dot(split_parts(field), gx)
            for h, half in enumerate(halves):
                half[where, :] = field[:, h * 128 : (h + 1) * 128]
        return carry

    lax.fori_loop(0, vec_count // 2, step, 0)
    for c in range(col_devices):
        for h, half in enumerate(halves):
            rows[h * 128 : (h + 1) * 128, :] = half[c * zv_length : (c + 1) * zv_length, :].T
        for r in range(row_devices):
            o_ref[r, c] = rows[r * x_length : (r + 1) * x_length, :]


def linear_terms(planes, speed, tables, vec_count):
    row_devices, col_devices, x_length, zv_length = planes.shape
    padded = tables[0].shape[0]
    z_count = tables[1].shape[0]
    flops = 2 * vec_count * 3 * 2 * (z_count * padded * padded + z_count * z_count * padded)
    return pl.pallas_call(
        functools.partial(plane_kernel, vec_count),
        out_shape=jax.ShapeDtypeStruct(planes.shape, jnp.float32),
        in_specs=[pl.BlockSpec(memory_space=pltpu.VMEM)] * 6,
        out_specs=pl.BlockSpec(memory_space=pltpu.VMEM),
        scratch_shapes=[pltpu.VMEM((padded, zv_length), jnp.float32)]
        + [pltpu.VMEM((z_count * vec_count, 128), jnp.float32)] * (padded // 128),
        cost_estimate=pl.CostEstimate(
            flops=flops, bytes_accessed=8 * planes.size, transcendentals=0
        ),
        compiler_params=pltpu.CompilerParams(vmem_limit_bytes=48 * 1024 * 1024),
    )(planes, speed, *tables)


def solve_kernel(chunks, q_ref, mask_ref, wave_ref, decay_ref, to_ref, from_ref, *rest):
    terms, (stepped_ref, gram_ref) = rest[:chunks], rest[chunks:]

    @pl.when(pl.program_id(0) == 0)
    def _():
        gram_ref[...] = jnp.zeros_like(gram_ref)

    nonlinear = jnp.concatenate([term[0] for term in terms], axis=0)
    right_side = STEP_COEF * q_ref[0] + nonlinear * mask_ref[0]
    eigen_part = parts_dot(split_parts(to_ref[...]), split_parts(right_side))
    eigen_part = eigen_part / (wave_ref[0] + decay_ref[...])
    stepped = parts_dot(split_parts(from_ref[...]), split_parts(eigen_part))
    stepped_ref[0] = stepped
    total = gram_ref[...]
    for g in range(stepped.shape[1] // 128):
        piece = stepped[:, g * 128 : (g + 1) * 128]
        total += lax.dot_general(
            piece,
            piece,
            (((0,), (0,)), ((), ())),
            precision=PRECISE,
            preferred_element_type=jnp.float32,
        )
    gram_ref[...] = total


def solve(tangents, mask_row, wave_row, decay_rates, to_eigen, from_eigen, terms):
    x_length, y_count, zv_length = tangents.shape
    whole = lambda *shape: pl.BlockSpec(shape, lambda m: (0,) * len(shape))
    one = lambda *shape: pl.BlockSpec((1,) + shape, lambda m: (m, 0, 0))
    return pl.pallas_call(
        functools.partial(solve_kernel, len(terms)),
        grid=(x_length,),
        out_shape=(
            jax.ShapeDtypeStruct(tangents.shape, jnp.float32),
            jax.ShapeDtypeStruct((128, 128), jnp.float32),
        ),
        in_specs=[
            one(y_count, zv_length),
            one(1, zv_length),
            one(1, zv_length),
            whole(y_count, 1),
            whole(y_count, y_count),
            whole(y_count, y_count),
        ]
        + [one(y_count // len(terms), zv_length)] * len(terms),
        out_specs=(one(y_count, zv_length), whole(128, 128)),
        compiler_params=pltpu.CompilerParams(vmem_limit_bytes=40 * 1024 * 1024),
    )(tangents, mask_row, wave_row, decay_rates[:, None], to_eigen, from_eigen, *terms)


def combine_kernel(x_ref, w_ref, o_ref):
    weights = split_parts(w_ref[...])
    for g in range(x_ref.shape[2] // 128):
        lanes = slice(g * 128, (g + 1) * 128)
        o_ref[0, :, lanes] = parts_dot(split_parts(x_ref[0, :, lanes]), weights)


def combine(stepped, weights):
    x_length, y_count, zv_length = stepped.shape
    one = pl.BlockSpec((1, y_count, zv_length), lambda m: (m, 0, 0))
    return pl.pallas_call(
        combine_kernel,
        grid=(x_length,),
        out_shape=jax.ShapeDtypeStruct(stepped.shape, jnp.float32),
        in_specs=[one, pl.BlockSpec((128, 128), lambda m: (0, 0))],
        out_specs=one,
    )(stepped, weights)


def body(tangents, base_flow, mode_mask, decay_rates, to_eigen, from_eigen):
    x_length, y_count, zv_length = tangents.shape
    z_length = base_flow.shape[2]
    vec_count = zv_length // z_length
    row_devices = lax.axis_size("row")
    col_devices = lax.axis_size("col")
    x_count = x_length * row_devices
    z_count = z_length * col_devices
    all_devices = row_devices * col_devices
    chunks = y_count // all_devices
    axes = ("row", "col")
    x_synthesis = synthesis(x_count)
    z_synthesis = synthesis(z_count)
    padded = -(-x_count // 128) * 128
    extra = padded - x_count
    widen = lambda table: jnp.pad(table, ((0, extra), (0, extra)))
    tables = (
        widen(x_synthesis.T),
        z_synthesis,
        analysis(z_count),
        widen(derivative_analysis(x_count, ALPHA_X).T),
    )
    exchange = lambda block: lax.all_to_all(block, axes, split_axis=0, concat_axis=0, tiled=True)
    base = jnp.transpose(base_flow.reshape(x_length, chunks, all_devices, z_length), (2, 1, 0, 3))
    base = exchange(base.reshape(all_devices, 1, chunks * x_length * z_length))
    base = base.reshape(row_devices, col_devices, chunks, x_length, z_length)
    base = jnp.transpose(base, (2, 0, 3, 1, 4)).reshape(chunks, x_count, z_count)
    speed = jnp.einsum("kmn,pm->kpn", base, x_synthesis, precision=PRECISE)
    speed = jnp.einsum("kpn,sn->ksp", speed, z_synthesis, precision=PRECISE)
    speed = jnp.pad(speed, ((0, 0), (0, 0), (0, extra)))
    received = []
    for k in range(chunks):
        piece = tangents[:, k * all_devices : (k + 1) * all_devices, :]
        received.append(exchange(jnp.transpose(piece, (1, 0, 2))))
    terms = []
    for k in range(chunks):
        planes = received[k].reshape(row_devices, col_devices, x_length, zv_length)
        returned = linear_terms(planes, speed[k], tables, vec_count)
        returned = exchange(returned.reshape(all_devices, x_length, zv_length))
        terms.append(jnp.transpose(returned, (1, 0, 2)))
    wave_x = ALPHA_X * local_waves(x_count, lax.axis_index("row") * x_length, x_length)
    wave_z = BETA_Z * local_waves(z_count, lax.axis_index("col") * z_length, z_length)
    wave_row = STEP_COEF + VISCOSITY * (wave_x[:, None] ** 2 + wave_z[None, :] ** 2)
    wave_row = jnp.repeat(wave_row, vec_count, axis=1)[:, None, :]
    mask_row = jnp.repeat(mode_mask.astype(jnp.float32), vec_count, axis=1)[:, None, :]
    stepped, local_gram = solve(
        tangents, mask_row, wave_row, decay_rates, to_eigen, from_eigen, terms
    )
    groups = 128 // vec_count
    local_gram = sum(
        local_gram[g * vec_count : (g + 1) * vec_count, g * vec_count : (g + 1) * vec_count]
        for g in range(groups)
    )
    gram_matrix = lax.psum(local_gram, axes) / (x_count * y_count * z_count)
    lower_factor = jnp.linalg.cholesky(gram_matrix)
    identity = jnp.eye(vec_count, dtype=jnp.float32)
    inverse = jax.scipy.linalg.solve_triangular(lower_factor, identity, lower=True)
    weights = jnp.kron(jnp.eye(groups, dtype=jnp.float32), inverse.T)
    return combine(stepped, weights), jnp.log(jnp.diagonal(lower_factor))


def solution(mesh):
    placed = (P("row", None, "col"), P("row", None, "col"), P("row", "col"), P(), P(), P())
    return jax.shard_map(
        body, mesh=mesh, in_specs=placed, out_specs=(P("row", None, "col"), P()), check_vma=False
    )
```

```python
import functools
import math

import jax
import jax.numpy as jnp
from jax import lax
from jax.experimental import pallas as pl
from jax.experimental.pallas import tpu as pltpu
from jax.sharding import PartitionSpec as P


PRECISE = lax.Precision.HIGHEST
STEP_COEF = 10.0
VISCOSITY = 0.01
ALPHA_X = 0.5
BETA_Z = 1.0


def local_waves(points_count, first_index, length):
    indices = first_index + jnp.arange(length, dtype=jnp.int32)
    middle = points_count // 2
    return jnp.where(indices <= middle, indices, indices - middle).astype(jnp.float32)


def synthesis(points_count):
    points = jnp.arange(points_count, dtype=jnp.int32)[:, None]
    mode_index = jnp.arange(points_count, dtype=jnp.int32)[None, :]
    middle = points_count // 2
    wave_index = jnp.where(mode_index <= middle, mode_index, mode_index - middle)
    turn_count = (points * wave_index % points_count).astype(jnp.float32)
    angles = turn_count * (2.0 * math.pi / points_count)
    return jnp.where(mode_index <= middle, jnp.cos(angles), jnp.sin(angles))


def analysis(points_count):
    mode_index = jnp.arange(points_count, dtype=jnp.int32)
    middle = points_count // 2
    weights = jnp.where(
        (mode_index == 0) | (mode_index == middle),
        jnp.float32(1.0 / points_count),
        jnp.float32(2.0 / points_count),
    )
    return weights[:, None] * synthesis(points_count).T


def derivative_analysis(points_count, wave_scale):
    rows_index = jnp.arange(points_count, dtype=jnp.int32)[:, None]
    cols_index = jnp.arange(points_count, dtype=jnp.int32)[None, :]
    middle = points_count // 2
    rising = (cols_index == rows_index + middle) & (rows_index >= 1) & (rows_index < middle)
    falling = (rows_index == cols_index + middle) & (cols_index >= 1) & (cols_index < middle)
    rows_float = jnp.broadcast_to(rows_index.astype(jnp.float32), (points_count, points_count))
    cols_float = jnp.broadcast_to(cols_index.astype(jnp.float32), (points_count, points_count))
    derivative = jnp.where(rising, rows_float, jnp.float32(0.0)) - jnp.where(
        falling, cols_float, jnp.float32(0.0)
    )
    return -wave_scale * jnp.dot(derivative, analysis(points_count), precision=PRECISE)


def split_parts(value):
    high = value.astype(jnp.bfloat16)
    low = (value - high.astype(jnp.float32)).astype(jnp.bfloat16)
    return high, low


def parts_dot(left, right):
    left_high, left_low = left
    right_high, right_low = right
    dot = lambda a, b: jnp.dot(a, b, preferred_element_type=jnp.float32)
    return dot(left_high, right_high) + (dot(left_high, right_low) + dot(left_low, right_high))


def plane_kernel(vec_count, x_ref, speed_ref, sx_ref, sz_ref, az_ref, gx_ref, o_ref, rows, *halves):
    row_devices, col_devices, _, x_length, zv_length = x_ref.shape
    x_count = row_devices * x_length
    z_count = sz_ref.shape[0]
    if rows.shape[0] > x_count:
        rows[x_count:, :] = jnp.zeros((rows.shape[0] - x_count, zv_length), jnp.float32)
    for c in range(col_devices):
        for r in range(row_devices):
            rows[r * x_length : (r + 1) * x_length, :] = x_ref[r, c, 0]
        for h, half in enumerate(halves):
            half[c * zv_length : (c + 1) * zv_length, :] = rows[h * 128 : (h + 1) * 128, :].T
    sx = split_parts(sx_ref[...])
    sz = split_parts(sz_ref[...])
    az = split_parts(az_ref[...])
    gx = split_parts(gx_ref[...])

    def step(group, carry):
        for u in range(2):
            where = pl.ds(group * 2 + u, z_count, stride=vec_count)
            field = jnp.concatenate([half[where, :] for half in halves], axis=1)
            field = parts_dot(split_parts(field), sx)
            field = parts_dot(sz, split_parts(field))
            field = field * speed_ref[0]
            field = parts_dot(az, split_parts(field))
            field = parts_dot(split_parts(field), gx)
            for h, half in enumerate(halves):
                half[where, :] = field[:, h * 128 : (h + 1) * 128]
        return carry

    lax.fori_loop(0, vec_count // 2, step, 0)
    for c in range(col_devices):
        for h, half in enumerate(halves):
            rows[h * 128 : (h + 1) * 128, :] = half[c * zv_length : (c + 1) * zv_length, :].T
        for r in range(row_devices):
            o_ref[r, c, 0] = rows[r * x_length : (r + 1) * x_length, :]


def linear_terms(planes, speed, tables, vec_count):
    row_devices, col_devices, plane_count, x_length, zv_length = planes.shape
    padded = tables[0].shape[0]
    z_count = tables[1].shape[0]
    flops = 2 * plane_count * vec_count * 6 * z_count * padded * (padded + z_count)
    field = pl.BlockSpec(
        (row_devices, col_devices, 1, x_length, zv_length), lambda l: (0, 0, l, 0, 0)
    )
    return pl.pallas_call(
        functools.partial(plane_kernel, vec_count),
        grid=(plane_count,),
        out_shape=jax.ShapeDtypeStruct(planes.shape, jnp.float32),
        in_specs=[field, pl.BlockSpec((1,) + speed.shape[1:], lambda l: (l, 0, 0))]
        + [pl.BlockSpec(table.shape, lambda l: (0, 0)) for table in tables],
        out_specs=field,
        scratch_shapes=[pltpu.VMEM((padded, zv_length), jnp.float32)]
        + [pltpu.VMEM((z_count * vec_count, 128), jnp.float32)] * (padded // 128),
        cost_estimate=pl.CostEstimate(
            flops=flops, bytes_accessed=8 * planes.size, transcendentals=0
        ),
        compiler_params=pltpu.CompilerParams(vmem_limit_bytes=48 * 1024 * 1024),
    )(planes, speed, *tables)


def prepare_kernel(q_ref, mask_ref, to_ref, *rest):
    terms, o_ref = rest[:-1], rest[-1]
    right_side = STEP_COEF * q_ref[0]
    if terms:
        added = jnp.concatenate([term[0] for term in terms], axis=0) * mask_ref[0]
        known = added.shape[0]
        right_side = jnp.concatenate([right_side[:known] + added, right_side[known:]], axis=0)
    o_ref[0] = parts_dot(split_parts(to_ref[...]), split_parts(right_side))


def prepare(tangents, mask_row, to_eigen, terms):
    x_length, y_count, zv_length = tangents.shape
    one = lambda *shape: pl.BlockSpec((1,) + shape, lambda m: (m, 0, 0))
    return pl.pallas_call(
        prepare_kernel,
        grid=(x_length,),
        out_shape=jax.ShapeDtypeStruct(tangents.shape, jnp.float32),
        in_specs=[
            one(y_count, zv_length),
            one(1, zv_length),
            pl.BlockSpec((y_count, y_count), lambda m: (0, 0)),
        ]
        + [one(term.shape[1], zv_length) for term in terms],
        out_specs=one(y_count, zv_length),
        cost_estimate=pl.CostEstimate(
            flops=6 * y_count * tangents.size, bytes_accessed=10 * tangents.size, transcendentals=0
        ),
        compiler_params=pltpu.CompilerParams(vmem_limit_bytes=16 * 1024 * 1024),
    )(tangents, mask_row, to_eigen, *terms)


def finish_kernel(
    eigen_ref, mask_ref, wave_ref, decay_ref, to_ref, from_ref, term_ref, stepped_ref, high_ref, cross_ref
):
    @pl.when(pl.program_id(0) == 0)
    def _():
        high_ref[...] = jnp.zeros_like(high_ref)
        cross_ref[...] = jnp.zeros_like(cross_ref)

    into, back = split_parts(to_ref[...]), split_parts(from_ref[...])
    highs, lows = [], []
    for b in range(eigen_ref.shape[0]):
        late = parts_dot(into, split_parts(term_ref[b] * mask_ref[b]))
        eigen_part = (eigen_ref[b] + late) / (wave_ref[b] + decay_ref[...])
        stepped = parts_dot(back, split_parts(eigen_part))
        stepped_ref[b] = stepped
        high, low = split_parts(stepped)
        highs.append(high)
        lows.append(low)
    high, low = jnp.concatenate(highs, axis=0), jnp.concatenate(lows, axis=0)
    inner = lambda a, b: lax.dot_general(
        a, b, (((0,), (0,)), ((), ())), preferred_element_type=jnp.float32
    )
    high_total, cross_total = high_ref[...], cross_ref[...]
    for g in range(high.shape[1] // 128):
        lanes = slice(g * 128, (g + 1) * 128)
        high_total += inner(high[:, lanes], high[:, lanes])
        cross_total += inner(high[:, lanes], low[:, lanes])
    high_ref[...] = high_total
    cross_ref[...] = cross_total


def finish(eigen_sum, mask_row, wave_row, decay_rates, to_late, from_eigen, term):
    x_length, y_count, zv_length = eigen_sum.shape
    batch = 2 if x_length % 2 == 0 else 1
    whole = lambda *shape: pl.BlockSpec(shape, lambda m: (0,) * len(shape))
    some = lambda *shape: pl.BlockSpec((batch,) + shape, lambda m: (m, 0, 0))
    square = jax.ShapeDtypeStruct((128, 128), jnp.float32)
    stepped, high, cross = pl.pallas_call(
        finish_kernel,
        grid=(x_length // batch,),
        out_shape=(jax.ShapeDtypeStruct(eigen_sum.shape, jnp.float32), square, square),
        in_specs=[
            some(y_count, zv_length),
            some(1, zv_length),
            some(1, zv_length),
            whole(y_count, 1),
            whole(*to_late.shape),
            whole(y_count, y_count),
            some(term.shape[1], zv_length),
        ],
        out_specs=(some(y_count, zv_length), whole(128, 128), whole(128, 128)),
        compiler_params=pltpu.CompilerParams(vmem_limit_bytes=20 * 1024 * 1024),
    )(eigen_sum, mask_row, wave_row, decay_rates[:, None], to_late, from_eigen, term)
    return stepped, high + cross + cross.T


def combine_kernel(x_ref, w_ref, o_ref):
    weights = split_parts(w_ref[...])
    for g in range(x_ref.shape[2] // 128):
        lanes = slice(g * 128, (g + 1) * 128)
        o_ref[0, :, lanes] = parts_dot(split_parts(x_ref[0, :, lanes]), weights)


def combine(stepped, weights):
    x_length, y_count, zv_length = stepped.shape
    one = pl.BlockSpec((1, y_count, zv_length), lambda m: (m, 0, 0))
    return pl.pallas_call(
        combine_kernel,
        grid=(x_length,),
        out_shape=jax.ShapeDtypeStruct(stepped.shape, jnp.float32),
        in_specs=[one, pl.BlockSpec((128, 128), lambda m: (0, 0))],
        out_specs=one,
        compiler_params=pltpu.CompilerParams(vmem_limit_bytes=12 * 1024 * 1024),
    )(stepped, weights)


def body(tangents, base_flow, mode_mask, decay_rates, to_eigen, from_eigen):
    x_length, y_count, zv_length = tangents.shape
    z_length = base_flow.shape[2]
    vec_count = zv_length // z_length
    row_devices = lax.axis_size("row")
    col_devices = lax.axis_size("col")
    x_count = x_length * row_devices
    z_count = z_length * col_devices
    all_devices = row_devices * col_devices
    device_planes = y_count // all_devices
    per_chunk = 2 if device_planes % 2 == 0 else 1
    chunks = device_planes // per_chunk
    chunk_rows = per_chunk * all_devices
    axes = ("row", "col")
    x_synthesis = synthesis(x_count)
    z_synthesis = synthesis(z_count)
    padded = -(-x_count // 128) * 128
    extra = padded - x_count
    widen = lambda table: jnp.pad(table, ((0, extra), (0, extra)))
    tables = (
        widen(x_synthesis.T),
        z_synthesis,
        analysis(z_count),
        widen(derivative_analysis(x_count, ALPHA_X).T),
    )
    exchange = lambda block: lax.all_to_all(block, axes, split_axis=0, concat_axis=0, tiled=True)
    received = []
    source = tangents
    for k in range(chunks):
        piece = source[:, k * chunk_rows : (k + 1) * chunk_rows, :]
        piece = jnp.transpose(piece, (1, 0, 2)).reshape(all_devices, per_chunk * x_length, zv_length)
        if k == 0:
            source, piece = lax.optimization_barrier((source, piece))
        received.append(exchange(piece))
    base = base_flow.reshape(x_length, chunks, all_devices, per_chunk, z_length)
    base = jnp.transpose(base, (2, 1, 3, 0, 4))
    base = exchange(base.reshape(all_devices, 1, device_planes * x_length * z_length))
    base = base.reshape(row_devices, col_devices, device_planes, x_length, z_length)
    base = jnp.transpose(base, (2, 0, 3, 1, 4)).reshape(device_planes, x_count, z_count)
    speed = jnp.einsum("kmn,pm->kpn", base, x_synthesis, precision=PRECISE)
    speed = jnp.einsum("kpn,sn->ksp", speed, z_synthesis, precision=PRECISE)
    speed = jnp.pad(speed, ((0, 0), (0, 0), (0, extra)))
    speed = speed.reshape(chunks, per_chunk, z_count, padded)
    terms = []
    for k in range(chunks):
        planes = received[k].reshape(row_devices, col_devices, per_chunk, x_length, zv_length)
        returned = linear_terms(planes, speed[k], tables, vec_count)
        returned = exchange(returned.reshape(all_devices, per_chunk * x_length, zv_length))
        terms.append(jnp.transpose(returned.reshape(chunk_rows, x_length, zv_length), (1, 0, 2)))
    wave_x = ALPHA_X * local_waves(x_count, lax.axis_index("row") * x_length, x_length)
    wave_z = BETA_Z * local_waves(z_count, lax.axis_index("col") * z_length, z_length)
    wave_row = STEP_COEF + VISCOSITY * (wave_x[:, None] ** 2 + wave_z[None, :] ** 2)
    wave_row = jnp.repeat(wave_row, vec_count, axis=1)[:, None, :]
    mask_row = jnp.repeat(mode_mask.astype(jnp.float32), vec_count, axis=1)[:, None, :]
    eigen_sum = prepare(tangents, mask_row, to_eigen, terms[:-1])
    to_late = to_eigen[:, y_count - chunk_rows :]
    stepped, local_gram = finish(
        eigen_sum, mask_row, wave_row, decay_rates, to_late, from_eigen, terms[-1]
    )
    groups = 128 // vec_count
    local_gram = sum(
        local_gram[g * vec_count : (g + 1) * vec_count, g * vec_count : (g + 1) * vec_count]
        for g in range(groups)
    )
    gram_matrix = lax.psum(lax.psum(local_gram, "row"), "col") / (x_count * y_count * z_count)
    lower_factor = jnp.linalg.cholesky(gram_matrix)
    identity = jnp.eye(vec_count, dtype=jnp.float32)
    inverse = jax.scipy.linalg.solve_triangular(lower_factor, identity, lower=True)
    weights = jnp.kron(jnp.eye(groups, dtype=jnp.float32), inverse.T)
    return combine(stepped, weights), jnp.log(jnp.diagonal(lower_factor))


def solution(mesh):
    placed = (P("row", None, "col"), P("row", None, "col"), P("row", "col"), P(), P(), P())
    return jax.shard_map(
        body, mesh=mesh, in_specs=placed, out_specs=(P("row", None, "col"), P()), check_vma=False
    )
```
